256 devices in a mesh: groups: 4 (over y, x), tile: 64 (over z, core).
Axes of the slice: x: 2, y: 2, z: 32, core: 2. Of those that a mesh axis runs over, the one named last changes fastest.
The devices are a block of a 4x8x32 slice.
Arguments:
- tracer: float32 [256, 6, 8, 128, 128], P(('groups', 'tile')), parts along dimension 0, may hold values from -6 to 6
- courant_east: bfloat16 [256, 6, 8, 128, 128], P(('groups', 'tile')), parts along dimension 0, may hold values from -1.5 to 1.5
- courant_north: bfloat16 [256, 6, 8, 128, 128], P(('groups', 'tile')), parts along dimension 0, may hold values from -1.5 to 1.5
- diffusivity: bfloat16 [256, 6, 8, 128, 128], P(('groups', 'tile')), parts along dimension 0, may hold values from 0.049804688 to 5
- seam_table: int32 [6, 4, 3], replicated, may hold values from 0 to 5, as said below
Outputs:
- updated: float32 [256, 6, 8, 128, 128], P(('groups', 'tile')), parts along dimension 0
The draws below stay inside these ranges and needn't reach their ends.
There are 4 independent parts, one for each index of `groups`. The reference program is written for one: setup_inputs(seed, part) draws one part's arguments, and reference() takes and returns one part's arrays. A program takes and returns all parts, laid end to end along the dimension named above; an argument that names none is the same for every part. Nothing has to cross between parts.
Inputs may be any that keep to these rules, and one draw needn't show every extreme that they name: seam_table[p, e] = (q, f, r) names the edge f of panel q != p that borders edge e of panel p, and r is 1 where their edge indices run in opposite directions, 0 otherwise; the 24 edges form 12 pairs whose entries name each other with the same r, as on the faces of a cube ; edge 3 of panel 0 borders edge 3 of panel 1.
All inputs are finite; a program needn't handle non-finite values.
Results may differ from the reference program's by a relative error of at most 0.0003.
Values sent between devices are 32-bit elements; how exact they have to be, the bound alone decides.
A program may use at most 128 MiB of HBM per device.

```python
import math
import jax
import jax.numpy as jnp
from jax import lax

CT = 128
LEVELS = 8
PANELS = 6
DEPTH = 2
SIDE = 8
N_TILE = 64


def turn_axes(first_old, second_old, quarter):
    first_axis = jnp.where(quarter == 0, first_old, jnp.where(quarter == 1, second_old, jnp.where(quarter == 2, -first_old, -second_old)))
    second_axis = jnp.where(quarter == 0, second_old, jnp.where(quarter == 1, -first_old, jnp.where(quarter == 2, -second_old, first_old)))
    return (first_axis, second_axis)


def draw_seam_table(key, part):
    normals = jnp.array([[1, 0, 0], [0, 1, 0], [0, 0, 1], [-1, 0, 0], [0, -1, 0], [0, 0, -1]], jnp.int32)
    firsts = jnp.array([[0, 1, 0], [0, 0, 1], [1, 0, 0], [0, 0, 1], [1, 0, 0], [0, 1, 0]], jnp.int32)
    seconds = jnp.array([[0, 0, 1], [1, 0, 0], [0, 1, 0], [0, 1, 0], [0, 0, 1], [1, 0, 0]], jnp.int32)
    split_keys = jax.random.split(jax.random.fold_in(key, 11), 3)
    head_label = jax.random.randint(split_keys[0], (1,), 0, 6)
    quarter = jax.random.randint(split_keys[1], (6, 1), 0, 4)
    centre_zero = normals[head_label]
    first_zero, second_zero = turn_axes(firsts[head_label], seconds[head_label], quarter[0:1])
    centre_one = -first_zero
    first_one = -centre_zero
    second_one = -second_zero
    remaining = jnp.concatenate([-centre_zero, first_zero, second_zero, -second_zero], axis=0)
    remaining = remaining[jax.random.permutation(split_keys[2], 4)]
    same_face = jnp.all(remaining[:, None, :] == normals[None, :, :], axis=-1).astype(jnp.int32)
    rest_labels = jnp.sum(same_face * jnp.arange(6, dtype=jnp.int32)[None, :], axis=1)
    first_rest, second_rest = turn_axes(firsts[rest_labels], seconds[rest_labels], quarter[2:])
    centre = jnp.concatenate([centre_zero, centre_one, remaining], axis=0)
    first_axis = jnp.concatenate([first_zero, first_one, first_rest], axis=0)
    second_axis = jnp.concatenate([second_zero, second_one, second_rest], axis=0)
    middle = jnp.stack([centre - second_axis, centre + first_axis, centre + second_axis, centre - first_axis], axis=1).reshape(24, 3)
    heading = jnp.stack([first_axis, second_axis, first_axis, second_axis], axis=1).reshape(24, 3)
    panel_of = jnp.arange(24, dtype=jnp.int32) // 4
    matches = jnp.all(middle[:, None, :] == middle[None, :, :], axis=-1) & (panel_of[:, None] != panel_of[None, :])
    partner = jnp.sum(matches.astype(jnp.int32) * jnp.arange(24, dtype=jnp.int32)[None, :], axis=1)
    partner_heading = jnp.sum(matches.astype(jnp.int32)[:, :, None] * heading[None, :, :], axis=1)
    reversal = (jnp.sum(heading * partner_heading, axis=-1) < 0).astype(jnp.int32)
    return jnp.stack([partner // 4, partner % 4, reversal], axis=-1).reshape(6, 4, 3).astype(jnp.int32)


def steps_of(key, extent, pieces, least, top_value):
    factor_of = 1.0
    for position, blocks in pieces:
        heights = jax.random.uniform(jax.random.fold_in(jax.random.fold_in(key, 6), position), (blocks,), jnp.float32, least / len(pieces), top_value / len(pieces))
        factor_of = factor_of * jnp.repeat(jnp.exp(heights), extent[position] // blocks).reshape((-1,) + (1,) * (len(extent) - 1 - position))
    return factor_of


def bell_draw(own_key, shape, width, limit, cuts=(), held_as=jnp.bfloat16):
    result = jax.random.normal(own_key, shape, jnp.float32) * width
    if len(cuts) > 0:
        result = steps_of(own_key, shape, cuts, -0.22, 0.18) * result
    return jnp.clip(result, min=-limit, max=limit).astype(held_as)


def setup_inputs(seed: int = 0, part: int = 0) -> dict:
    arg_keys = jax.random.split(jax.random.key(seed), 6)
    own_keys = jax.random.split(jax.random.fold_in(arg_keys[5], part), 6)
    tracer = bell_draw(own_keys[0], (N_TILE, PANELS, LEVELS, CT, CT), 1.0, 6.0, ((0, 64),), jnp.float32)
    courant_east = bell_draw(own_keys[1], (N_TILE, PANELS, LEVELS, CT, CT), 0.3, 1.5, ((0, 64),))
    courant_north = bell_draw(own_keys[2], (N_TILE, PANELS, LEVELS, CT, CT), 0.3, 1.5, ((0, 64),))
    diffusivity = jnp.clip(jnp.exp(math.log(5.0) - 4.609084 * jax.random.uniform(own_keys[3], (N_TILE, PANELS, LEVELS, CT, CT), jnp.float32) ** steps_of(own_keys[3], (N_TILE, PANELS, LEVELS, CT, CT), ((0, 64),), -0.2, 0.2)), 0.049804688, 5.0).astype(jnp.bfloat16)
    seam_table = draw_seam_table(jax.random.fold_in(arg_keys[5], 71), part)
    return dict(tracer=tracer, courant_east=courant_east, courant_north=courant_north, diffusivity=diffusivity, seam_table=seam_table)


def edge_strips(panels, rows_deep):
    south_rows = jnp.moveaxis(panels[:, :, :, :rows_deep], 3, 1)
    east_rows = jnp.moveaxis(panels[:, :, ::-1, :][:, :, :rows_deep, :], 2, 1)
    north_rows = jnp.moveaxis(panels[:, :, :, ::-1][:, :, :, :rows_deep], 3, 1)
    west_rows = jnp.moveaxis(panels[:, :, :rows_deep, :], 2, 1)
    return jnp.stack([south_rows, east_rows, north_rows, west_rows], axis=1)


def centered(extended, along):
    kept = extended.shape[along] - 4

    def shifted(offset):
        return lax.slice_in_dim(extended, 2 + offset, 2 + offset + kept, axis=along)

    return (8.0 * (shifted(1) - shifted(-1)) - (shifted(2) - shifted(-2))) / 12.0


def advance(panels, ghosts, courant_east, courant_north, diffusivity):
    west_part = jnp.moveaxis(ghosts[:, 3, ::-1], 1, 2)
    east_part = jnp.moveaxis(ghosts[:, 1], 1, 2)
    south_part = jnp.transpose(ghosts[:, 0, ::-1], (0, 2, 3, 1))
    north_part = jnp.transpose(ghosts[:, 2], (0, 2, 3, 1))
    along_first = jnp.concatenate([west_part, panels, east_part], axis=2)
    along_second = jnp.concatenate([south_part, panels, north_part], axis=3)
    forced = panels - (courant_east.astype(jnp.float32) * centered(along_first, 2)
                       + courant_north.astype(jnp.float32) * centered(along_second, 3))
    coupling = diffusivity.astype(jnp.float32)
    ratios = []
    partial_values = []
    for height in range(panels.shape[1]):
        diagonal = 1.0 + coupling[:, height]
        if height > 0:
            below = coupling[:, height - 1]
            pivot_value = diagonal + below - below * ratios[-1]
            current = (forced[:, height] + below * partial_values[-1]) / pivot_value
        else:
            pivot_value = diagonal
            current = forced[:, height] / pivot_value
        ratios.append(coupling[:, height] / pivot_value)
        partial_values.append(current)
    solved = [partial_values[-1]]
    for height in range(panels.shape[1] - 2, -1, -1):
        solved.insert(0, partial_values[height] + ratios[height] * solved[0])
    return jnp.stack(solved, axis=1)


def panel_offset(panel_no):
    return (panel_no % 2) * (SIDE * SIDE // 2 + 1)


def to_panels(tiles):
    aligned = jnp.stack([jnp.roll(tiles[:, panel_no], -panel_offset(panel_no), axis=0)
                         for panel_no in range(PANELS)], axis=1)
    shaped = aligned.reshape(SIDE, SIDE, PANELS, LEVELS, CT, CT)
    shaped = jnp.transpose(shaped, (2, 3, 0, 4, 1, 5))
    return shaped.reshape(PANELS, LEVELS, SIDE * CT, SIDE * CT)


def to_tiles(panels):
    shaped = panels.reshape(PANELS, LEVELS, SIDE, CT, SIDE, CT)
    shaped = jnp.transpose(shaped, (2, 4, 0, 1, 3, 5))
    aligned = shaped.reshape(SIDE * SIDE, PANELS, LEVELS, CT, CT)
    return jnp.stack([jnp.roll(aligned[:, panel_no], panel_offset(panel_no), axis=0)
                      for panel_no in range(PANELS)], axis=1)


def reference(tracer, courant_east, courant_north, diffusivity, seam_table):
    panels = to_panels(tracer)
    strips = edge_strips(panels, DEPTH)
    flat_strips = strips.reshape((PANELS * 4,) + strips.shape[2:])
    source_block = (seam_table[:, :, 0] * 4 + seam_table[:, :, 1]).reshape(-1).astype(jnp.int32)
    reverse_it = (seam_table[:, :, 2] == 1).reshape(-1)
    picked = jnp.take(flat_strips, source_block, axis=0)
    picked = jnp.where(reverse_it[:, None, None, None], picked[..., ::-1], picked)
    ghosts = picked.reshape(strips.shape)
    updated = advance(panels, ghosts, to_panels(courant_east), to_panels(courant_north), to_panels(diffusivity))
    return to_tiles(updated)
```

```python
import functools
import math

import jax
import jax.numpy as jnp
from jax import lax
from jax.experimental import pallas as pl
from jax.experimental.pallas import tpu as pltpu
from jax.sharding import PartitionSpec as P

MESH = pl.DeviceIdType.MESH
PAD = 8


class Plan:
    def __init__(self, count):
        self.count = count
        self.side = math.isqrt(count)
        self.shift = count // 2 + 1
        taken = []
        for group in range(self.side // 2):
            members = {
                self.site(par, edge, spot)
                for par in range(2)
                for edge in range(4)
                for spot in (group, self.side - 1 - group)
            }
            free = (d for d in range(1, count, 2) if d not in members and d not in taken)
            taken.append(next(free))
        self.hubs = taken

    def site(self, par, edge, spot):
        side = self.side
        tile = (spot * side, (side - 1) * side + spot, spot * side + side - 1, spot)[edge]
        return (tile + self.shift * par) % self.count

    def hub_of(self, group):
        found = self.hubs[0]
        for i, hub in enumerate(self.hubs):
            if i:
                found = jnp.where(group == i, hub, found)
        return found


def kernel(
    plan, dims,
    tracer, east, north, diff, seam, out,
    q, ce, cn, df, fv, wv, vv, bv, rv,
    strips, turned, ghosts, held, chosen, gi, xb, tt,
    load_sem, coef_sem, send_sem, ghost_sem, held_sem, chosen_sem,
):
    panels, levels, size = dims
    count, side = plan.count, plan.side
    block = levels * size
    me = lax.axis_index("tile")
    half = panels // 2

    def device(d):
        return {"tile": d}

    tiles = [lax.rem(me + (count - plan.shift) * par, count) for par in range(2)]
    rows = [t // side for t in tiles]
    cols = [lax.rem(t, side) for t in tiles]
    on_edge, other, slot, hub, near = {}, {}, {}, {}, {}
    for par in range(2):
        for edge in range(4):
            key = par, edge
            on_edge[key] = (
                cols[par] == 0, rows[par] == side - 1, cols[par] == side - 1, rows[par] == 0
            )[edge]
            spot = (rows, cols, rows, cols)[edge][par]
            group = jnp.minimum(spot, side - 1 - spot)
            other[key] = jnp.where(spot == group, 0, 1)
            slot[key] = (par * 4 + edge) * 2 + other[key]
            hub[key] = plan.hub_of(group)
            near[key] = lax.rem(me + (count - 1, side, 1, count - side)[edge], count)

    barrier = pltpu.get_barrier_semaphore()
    for key in on_edge:
        @pl.when(jnp.logical_not(on_edge[key]))
        def _(key=key):
            pl.semaphore_signal(
                barrier, inc=1, device_id=device(near[key]), device_id_type=MESH
            )
    for group, hub_device in enumerate(plan.hubs):
        @pl.when(me == hub_device)
        def _(group=group):
            for par in range(2):
                for edge in range(4):
                    for spot in (group, side - 1 - group):
                        pl.semaphore_signal(
                            barrier, inc=1, device_id=device(plan.site(par, edge, spot)),
                            device_id_type=MESH,
                        )

    loads = []
    for p in range(panels):
        load = pltpu.make_async_copy(
            tracer.at[pl.ds(p * block, block)], q.at[pl.ds(PAD + p * block, block)],
            load_sem.at[p],
        )
        load.start()
        loads.append(load)
    coefs = []
    for p in range(panels):
        for i, (far, close) in enumerate(((east, ce), (north, cn), (diff, df))):
            load = pltpu.make_async_copy(
                far.at[pl.ds(p * block, block)], close.at[pl.ds(p * block, block)],
                coef_sem.at[p, i],
            )
            load.start()
            coefs.append(load)

    zero = jnp.zeros((8, size), jnp.float32)
    q[pl.ds(0, PAD), :] = zero
    q[pl.ds(PAD + panels * block, PAD), :] = zero
    gi[...] = jnp.zeros(gi.shape, jnp.float32)
    xb[...] = jnp.zeros(xb.shape, jnp.float32)
    lane = lax.broadcasted_iota(jnp.int32, (8, size), 1)
    back = size - 1 - lax.broadcasted_iota(jnp.int32, (2 * levels, size), 1)

    for p in range(panels):
        par, idx = p % 2, p // 2
        first = PAD + p * block
        loads[p].wait()

        def gather(i, carry):
            packed = jnp.zeros((8, size), jnp.float32)
            for k in range(levels):
                row = pl.multiple_of(first + k * size + i * 8, 8)
                moved = pltpu.roll(q[pl.ds(row, 8), :], 4 * k + 2, 1)
                packed = jnp.where(lane // 4 == k, moved, packed)
            tt[p, pl.ds(pl.multiple_of(i * 8, 8), 8), :] = packed
            return carry

        lax.fori_loop(0, size // 8, gather, 0, unroll=4)
        tt[p] = jnp.transpose(tt[p])
        for d in range(2):
            part = pl.ds(d * levels, levels)
            strips[par, 0, idx, part, :] = tt[p, pl.ds(2 + d, levels, stride=4), :]
            strips[par, 2, idx, part, :] = tt[p, pl.ds(1 - d, levels, stride=4), :]
            strips[par, 3, idx, part, :] = q[pl.ds(first + d, levels, stride=size), :]
            strips[par, 1, idx, part, :] = q[pl.ds(first + size - 1 - d, levels, stride=size), :]
        for edge in range(4):
            plain = strips[par, edge, idx]
            flipped = jnp.take_along_axis(plain, back, axis=1)
            turn = seam[2, edge, p]
            turned[par, edge, idx] = jnp.where(turn == 1, flipped, plain)

    def to_hub(key):
        par, edge = key
        return pltpu.make_async_remote_copy(
            turned.at[par, edge], held.at[pl.ds(slot[key] * half, half)],
            send_sem.at[par * 4 + edge], held_sem.at[slot[key]],
            device_id=device(hub[key]), device_id_type=MESH,
        )

    def to_near(key):
        par, edge = key
        return pltpu.make_async_remote_copy(
            strips.at[par, edge], ghosts.at[par, (edge + 2) % 4],
            send_sem.at[par * 4 + edge], ghost_sem.at[par * 4 + (edge + 2) % 4],
            device_id=device(near[key]), device_id_type=MESH,
        )

    pl.semaphore_wait(barrier, 8)
    for key in on_edge:
        @pl.when(on_edge[key])
        def _(key=key):
            to_hub(key).start()

        @pl.when(jnp.logical_not(on_edge[key]))
        def _(key=key):
            to_near(key).start()

    twelfth = 1.0 / 12.0
    wide = lax.broadcasted_iota(jnp.int32, (16, size), 1)
    edge_lane = jnp.logical_or(wide < 2, wide >= size - 2)

    for p in range(panels):
        for load in coefs[3 * p : 3 * p + 3]:
            load.wait()

        def prepare(i, carry):
            before = ratio = None
            for k in range(levels):
                row = pl.multiple_of(p * block + k * size + i * 16, 16)
                here = pl.ds(row, 16)
                mid = q[pl.ds(row + PAD, 16), :]
                di = 8.0 * (q[pl.ds(row + PAD + 1, 16), :] - q[pl.ds(row + PAD - 1, 16), :]) - (
                    q[pl.ds(row + PAD + 2, 16), :] - q[pl.ds(row + PAD - 2, 16), :]
                )
                dj = 8.0 * (pltpu.roll(mid, size - 1, 1) - pltpu.roll(mid, 1, 1)) - (
                    pltpu.roll(mid, size - 2, 1) - pltpu.roll(mid, 2, 1)
                )
                e = ce[here, :].astype(jnp.float32) * twelfth
                n = cn[here, :].astype(jnp.float32) * twelfth
                c = df[here, :].astype(jnp.float32)
                pivot = 1.0 + c
                if k:
                    pivot = pivot + before * (1.0 - ratio)
                inv = 1.0 / pivot
                fv[here, :] = (mid - (e * di + n * dj)) * inv
                wv[here, :] = jnp.where(edge_lane, n * inv, 0.0)
                vv[here, :] = e * inv
                if k:
                    bv[here, :] = before * inv
                ratio = c * inv
                rv[here, :] = ratio
                before = c
            return carry

        lax.fori_loop(0, size // 16, prepare, 0)

    for group, hub_device in enumerate(plan.hubs):
        @pl.when(me == hub_device)
        def _(group=group):
            sites = [
                (par, edge, hi) for par in range(2) for edge in range(4) for hi in range(2)
            ]

            def to_site(number):
                par, edge, hi = sites[number]
                target = plan.site(par, edge, side - 1 - group if hi else group)
                return pltpu.make_async_remote_copy(
                    chosen.at[pl.ds(number * half, half)], ghosts.at[par, edge],
                    chosen_sem.at[number], ghost_sem.at[par * 4 + edge],
                    device_id=device(target), device_id_type=MESH,
                )

            for number in range(len(sites)):
                pltpu.make_async_remote_copy(
                    held.at[pl.ds(number * half, half)], held.at[pl.ds(number * half, half)],
                    chosen_sem.at[number], held_sem.at[number],
                    device_id=device(0), device_id_type=MESH,
                ).wait_recv()
            for number, (par, edge, hi) in enumerate(sites):
                for idx in range(half):
                    far_panel, far_edge, turn = (seam[i, edge, 2 * idx + par] for i in range(3))
                    far_hi = hi + turn - 2 * hi * turn
                    source = ((far_panel % 2) * 4 + far_edge) * 2 + far_hi
                    chosen[number * half + idx] = held[source * half + far_panel // 2]
                to_site(number).start()
            for number in range(len(sites)):
                to_site(number).wait_send()

    for key in on_edge:
        par, edge = key
        pltpu.make_async_remote_copy(
            strips.at[par, edge], ghosts.at[par, edge],
            send_sem.at[par * 4 + edge], ghost_sem.at[par * 4 + edge],
            device_id=device(near[key]), device_id_type=MESH,
        ).wait_recv()

    for p in range(panels):
        par, idx = p % 2, p // 2
        first = PAD + p * block

        def beyond(edge, d):
            return ghosts[par, edge, idx, pl.ds(d * levels, levels), :]

        def own(edge, d):
            return strips[par, edge, idx, pl.ds(d * levels, levels), :]

        low = [beyond(0, d) - own(2, d) for d in range(2)]
        high = [beyond(2, d) - own(0, d) for d in range(2)]
        for m, value in enumerate(
            (-high[0], 8.0 * high[0] - high[1], low[1] - 8.0 * low[0], low[0])
        ):
            xb[pl.ds(m, levels, stride=4), :] = value
        tt[p] = jnp.transpose(xb[...])

        low = [beyond(3, d) - q[pl.ds(first - 1 - d, levels, stride=size), :] for d in range(2)]
        high = [beyond(1, d) - q[pl.ds(first + size + d, levels, stride=size), :] for d in range(2)]
        base = p * 2 * levels * 8
        gi[pl.ds(base, levels, stride=8), :] = low[1] - 8.0 * low[0]
        gi[pl.ds(base + 1, levels, stride=8), :] = low[0]
        base = base + levels * 8
        gi[pl.ds(base + 6, levels, stride=8), :] = -high[0]
        gi[pl.ds(base + 7, levels, stride=8), :] = 8.0 * high[0] - high[1]

        for k in range(levels):
            for last in range(2):
                here = pl.ds(p * block + k * size + last * (size - 8), 8)
                change = gi[pl.ds(((p * 2 + last) * levels + k) * 8, 8), :]
                fv[here, :] = fv[here, :] - vv[here, :] * change

    def finish(step, carry):
        p = step // (size // 16)
        i = lax.rem(step, size // 16)
        fix = tt[p, pl.ds(pl.multiple_of(i * 16, 16), 16), :]
        values, places = [], []
        for k in range(levels):
            here = pl.ds(pl.multiple_of(p * block + k * size + i * 16, 16), 16)
            value = fv[here, :] - wv[here, :] * pltpu.roll(fix, size - (4 * k + 2), 1)
            if k:
                value = value + bv[here, :] * values[-1]
            values.append(value)
            places.append(here)
        above = values[-1]
        out[places[-1], :] = above
        for k in range(levels - 2, -1, -1):
            above = values[k] + rv[places[k], :] * above
            out[places[k], :] = above
        return carry

    lax.fori_loop(0, panels * (size // 16), finish, 0)

    for key in on_edge:
        @pl.when(on_edge[key])
        def _(key=key):
            to_hub(key).wait_send()

        @pl.when(jnp.logical_not(on_edge[key]))
        def _(key=key):
            to_near(key).wait_send()


def shards(plan, tracer, east, north, diff, seam):
    _, panels, levels, size, _ = tracer.shape
    dims = panels, levels, size
    total = panels * levels * size
    half = panels // 2
    f32, bf16 = jnp.float32, jnp.bfloat16
    anywhere = pl.BlockSpec(memory_space=pltpu.HBM)
    edge_set = pltpu.VMEM((2, 4, half, 2 * levels, size), f32)
    hub_set = pltpu.VMEM((16 * half, 2 * levels, size), f32)
    whole = pltpu.VMEM((total, size), f32)
    updated = pl.pallas_call(
        functools.partial(kernel, plan, dims),
        out_shape=pltpu.VMEM((total, size), f32),
        in_specs=[anywhere] * 4 + [pl.BlockSpec(memory_space=pltpu.SMEM)],
        out_specs=pl.BlockSpec(memory_space=pltpu.VMEM),
        scratch_shapes=[
            pltpu.VMEM((total + 2 * PAD, size), f32),
            *[pltpu.VMEM((total, size), bf16)] * 3,
            *[whole] * 5,
            *[edge_set] * 3,
            *[hub_set] * 2,
            pltpu.VMEM((panels * 2 * levels * 8, size), f32),
            pltpu.VMEM((size, size), f32),
            pltpu.VMEM((panels, size, size), f32),
            pltpu.SemaphoreType.DMA((panels,)),
            pltpu.SemaphoreType.DMA((panels, 3)),
            pltpu.SemaphoreType.DMA((8,)),
            pltpu.SemaphoreType.DMA((8,)),
            pltpu.SemaphoreType.DMA((16,)),
            pltpu.SemaphoreType.DMA((16,)),
        ],
        compiler_params=pltpu.CompilerParams(
            collective_id=0, has_side_effects=True, vmem_limit_bytes=40 * 1024 * 1024
        ),
        name="transport",
    )(
        *[
            pltpu.with_memory_space_constraint(value, pltpu.HBM)
            for value in (
                *[field.reshape(total, size) for field in (tracer, east, north, diff)],
                jnp.transpose(seam, (2, 1, 0)),
            )
        ]
    )
    return updated.reshape(tracer.shape)


def solution(mesh):
    plan = Plan(mesh.shape["tile"])
    spread = P(("groups", "tile"), None, None, None, None)
    return jax.shard_map(
        functools.partial(shards, plan),
        mesh=mesh,
        in_specs=(spread, spread, spread, spread, P()),
        out_specs=spread,
        check_vma=False,
    )
```

```python
import functools
import math

import jax
import jax.numpy as jnp
from jax import lax
from jax.experimental import pallas as pl
from jax.experimental.pallas import tpu as pltpu
from jax.sharding import PartitionSpec as P

MESH = pl.DeviceIdType.MESH
PAD = 8


class Plan:
    def __init__(self, count):
        self.count = count
        self.side = math.isqrt(count)
        self.shift = count // 2 + 1
        taken = []
        for group in range(self.side // 2):
            members = {self.site(*place) for place in self.places(group)}
            taken.append(
                next(d for d in range(1, count, 2) if d not in members and d not in taken)
            )
        self.hubs = taken

    def places(self, group):
        spots = group, self.side - 1 - group
        return [(par, edge, spot) for par in range(2) for edge in range(4) for spot in spots]

    def order(self, group):
        homes = [self.site(*place) for place in self.places(group)]
        return sorted(range(len(homes)), key=lambda i: (homes[i] >= 3 * self.count // 4, homes[i]))

    def site(self, par, edge, spot):
        side = self.side
        tile = (spot * side, (side - 1) * side + spot, spot * side + side - 1, spot)[edge]
        return (tile + self.shift * par) % self.count

    def hub_of(self, group):
        found = self.hubs[0]
        for i, hub in enumerate(self.hubs):
            if i:
                found = jnp.where(group == i, hub, found)
        return found


def kernel(
    plan, dims,
    tracer, slabs, east, north, diff, table, out,
    seam, rim, q, ce, cn, df, fv, wv, vv, bv, rv,
    strips, turned, ghosts, held, chosen, gi, xb, tt,
    table_sem, rim_sem, load_sem, coef_sem, send_sem, ghost_sem, held_sem, chosen_sem,
):
    panels, levels, size = dims
    count, side = plan.count, plan.side
    block = levels * size
    me = lax.axis_index("tile")
    half = panels // 2

    def device(d):
        return {"tile": d}

    tiles = [lax.rem(me + (count - plan.shift) * par, count) for par in range(2)]
    rows = [t // side for t in tiles]
    cols = [lax.rem(t, side) for t in tiles]
    on_edge, below, above_me, slot, hub, near = {}, {}, {}, {}, {}, {}
    for par in range(2):
        for edge in range(4):
            key = par, edge
            on_edge[key] = (
                cols[par] == 0, rows[par] == side - 1, cols[par] == side - 1, rows[par] == 0
            )[edge]
            spot = (rows, cols, rows, cols)[edge][par]
            group = jnp.minimum(spot, side - 1 - spot)
            slot[key] = (par * 4 + edge) * 2 + jnp.where(spot == group, 0, 1)
            hub[key] = plan.hub_of(group)
            near[key] = lax.rem(me + (count - 1, side, 1, count - side)[edge], count)
            inside = jnp.logical_not(on_edge[key])
            below[key] = jnp.logical_and(inside, near[key] < me)
            above_me[key] = jnp.logical_and(inside, near[key] > me)

    barrier = pltpu.get_barrier_semaphore()
    expected = 0
    for key in on_edge:
        expected = expected + jnp.where(jnp.logical_or(on_edge[key], below[key]), 1, 0)

        @pl.when(above_me[key])
        def _(key=key):
            pl.semaphore_signal(
                barrier, inc=1, device_id=device(near[key]), device_id_type=MESH
            )
    for group, hub_device in enumerate(plan.hubs):
        @pl.when(me == hub_device)
        def _(group=group):
            for place in plan.places(group):
                pl.semaphore_signal(
                    barrier, inc=1, device_id=device(plan.site(*place)), device_id_type=MESH
                )

    table_load = pltpu.make_async_copy(table, seam, table_sem)
    table_load.start()
    rim_loads = [
        pltpu.make_async_copy(slabs.at[:, pl.ds(start, 8), :], rim.at[i], rim_sem.at[i])
        for i, start in enumerate((0, size - 8))
    ]
    for load in rim_loads:
        load.start()
    loads = []
    for p in range(panels):
        load = pltpu.make_async_copy(
            tracer.at[pl.ds(p * block, block)], q.at[pl.ds(PAD + p * block, block)],
            load_sem.at[p],
        )
        load.start()
        loads.append(load)
    coefs = [
        pltpu.make_async_copy(
            far.at[pl.ds(p * block, block)], close.at[pl.ds(p * block, block)],
            coef_sem.at[p, i],
        )
        for p in range(panels)
        for i, (far, close) in enumerate(((east, ce), (north, cn), (diff, df)))
    ]

    zero = jnp.zeros((8, size), jnp.float32)
    q[pl.ds(0, PAD), :] = zero
    q[pl.ds(PAD + panels * block, PAD), :] = zero
    gi[...] = jnp.zeros(gi.shape, jnp.float32)
    xb[...] = jnp.zeros(xb.shape, jnp.float32)
    lane = lax.broadcasted_iota(jnp.int32, (8, size), 1)
    back = size - 1 - lax.broadcasted_iota(jnp.int32, (2 * levels, size), 1)

    def turn_strips(p, edges):
        par, idx = p % 2, p // 2
        for edge in edges:
            plain = strips[par, edge, idx]
            flipped = jnp.take_along_axis(plain, back, axis=1)
            turned[par, edge, idx] = jnp.where(seam[2, edge, p] == 1, flipped, plain)

    for load in rim_loads:
        load.wait()
    table_load.wait()
    for p in range(panels):
        par, idx = p % 2, p // 2
        for d in range(2):
            part = pl.ds(d * levels, levels)
            strips[par, 3, idx, part, :] = rim[0, pl.ds(p * levels, levels), d, :]
            strips[par, 1, idx, part, :] = rim[1, pl.ds(p * levels, levels), 7 - d, :]
    for p in range(panels):
        turn_strips(p, (1, 3))

    def to_hub(key):
        par, edge = key
        return pltpu.make_async_remote_copy(
            turned.at[par, edge], held.at[pl.ds(slot[key] * half, half)],
            send_sem.at[par * 4 + edge], held_sem.at[slot[key]],
            device_id=device(hub[key]), device_id_type=MESH,
        )

    def to_near(key):
        par, edge = key
        return pltpu.make_async_remote_copy(
            strips.at[par, edge], ghosts.at[par, (edge + 2) % 4],
            send_sem.at[par * 4 + edge], ghost_sem.at[par * 4 + (edge + 2) % 4],
            device_id=device(near[key]), device_id_type=MESH,
        )

    def arrival(par, edge):
        return pltpu.make_async_remote_copy(
            strips.at[par, edge], ghosts.at[par, edge],
            send_sem.at[par * 4 + edge], ghost_sem.at[par * 4 + edge],
            device_id=device(0), device_id_type=MESH,
        )

    def send(edges):
        keys = [(par, edge) for edge in edges for par in range(2)]
        for key in keys:
            @pl.when(on_edge[key])
            def _(key=key):
                to_hub(key).start()

        for key in keys:
            @pl.when(below[key])
            def _(key=key):
                to_near(key).start()

    pl.semaphore_wait(barrier, expected)
    send((1, 3))

    for load in loads:
        load.wait()
    for load in coefs:
        load.start()
    part_of = lane // 4
    for p in range(panels):
        for i in range(size // 8):
            packed = jnp.zeros((8, size), jnp.float32)
            for k in range(levels):
                moved = pltpu.roll(
                    q[pl.ds(PAD + p * block + k * size + i * 8, 8), :], 4 * k + 2, 1
                )
                packed = jnp.where(part_of == k, moved, packed)
            tt[p, pl.ds(i * 8, 8), :] = packed
    for p in range(panels):
        tt[p] = jnp.transpose(tt[p])
    for p in range(panels):
        par, idx = p % 2, p // 2
        for d in range(2):
            part = pl.ds(d * levels, levels)
            strips[par, 0, idx, part, :] = tt[p, pl.ds(2 + d, levels, stride=4), :]
            strips[par, 2, idx, part, :] = tt[p, pl.ds(1 - d, levels, stride=4), :]
    for p in range(panels):
        turn_strips(p, (0, 2))

    send((0, 2))

    twelfth = 1.0 / 12.0
    wide = lax.broadcasted_iota(jnp.int32, (16, size), 1)
    edge_lane = jnp.logical_or(wide < 2, wide >= size - 2)

    for p in range(panels):
        for load in coefs[3 * p : 3 * p + 3]:
            load.wait()

        def prepare(i, carry):
            before = ratio = None
            for k in range(levels):
                row = pl.multiple_of(p * block + k * size + i * 16, 16)
                here = pl.ds(row, 16)
                mid = q[pl.ds(row + PAD, 16), :]
                di = 8.0 * (q[pl.ds(row + PAD + 1, 16), :] - q[pl.ds(row + PAD - 1, 16), :]) - (
                    q[pl.ds(row + PAD + 2, 16), :] - q[pl.ds(row + PAD - 2, 16), :]
                )
                dj = 8.0 * (pltpu.roll(mid, size - 1, 1) - pltpu.roll(mid, 1, 1)) - (
                    pltpu.roll(mid, size - 2, 1) - pltpu.roll(mid, 2, 1)
                )
                e = ce[here, :].astype(jnp.float32) * twelfth
                n = cn[here, :].astype(jnp.float32) * twelfth
                c = df[here, :].astype(jnp.float32)
                pivot = 1.0 + c
                if k:
                    pivot = pivot + before * (1.0 - ratio)
                inv = 1.0 / pivot
                fv[here, :] = (mid - (e * di + n * dj)) * inv
                wv[here, :] = jnp.where(edge_lane, n * inv, 0.0)
                vv[here, :] = e * inv
                if k:
                    bv[here, :] = before * inv
                ratio = c * inv
                rv[here, :] = ratio
                before = c
            return carry

        lax.fori_loop(0, size // 16, prepare, 0)

    def send_up(around):
        for key in on_edge:
            far = near[key] - me > count // 2
            @pl.when(jnp.logical_and(above_me[key], far if around else jnp.logical_not(far)))
            def _(key=key):
                arrival(*key).wait_recv()
                to_near(key).start()

    send_up(False)

    def to_site(group, i):
        par, edge, _ = place = plan.places(group)[i]
        return pltpu.make_async_remote_copy(
            chosen.at[pl.ds(i * half, half)], ghosts.at[par, edge],
            chosen_sem.at[i], ghost_sem.at[par * 4 + edge],
            device_id=device(plan.site(*place)), device_id_type=MESH,
        )

    for group, hub_device in enumerate(plan.hubs):
        @pl.when(me == hub_device)
        def _(group=group):
            places = plan.places(group)
            for i in range(len(places)):
                pltpu.make_async_remote_copy(
                    held.at[pl.ds(i * half, half)], held.at[pl.ds(i * half, half)],
                    chosen_sem.at[i], held_sem.at[i],
                    device_id=device(0), device_id_type=MESH,
                ).wait_recv()
            for i in plan.order(group):
                par, edge, spot = places[i]
                mirrored = int(spot != group)
                for idx in range(half):
                    far_panel, far_edge, turn = (seam[j, edge, 2 * idx + par] for j in range(3))
                    far_mirrored = mirrored + turn - 2 * mirrored * turn
                    source = ((far_panel % 2) * 4 + far_edge) * 2 + far_mirrored
                    chosen[i * half + idx] = held[source * half + far_panel // 2]
                to_site(group, i).start()

    send_up(True)

    bent = functools.reduce(jnp.logical_or, [on_edge[0, edge] for edge in range(4)])

    def solve(par):
        for edge in range(4):
            late = jnp.logical_not(jnp.where(par == 0, above_me[0, edge], above_me[1, edge]))

            @pl.when(late)
            def _(edge=edge):
                arrival(par, edge).wait_recv()

        for idx in range(half):
            p = 2 * idx + par
            first = pl.multiple_of(PAD + p * block, 8)

            def beyond(edge, d):
                return ghosts[par, edge, idx, pl.ds(d * levels, levels), :]

            def own(edge, d):
                return strips[par, edge, idx, pl.ds(d * levels, levels), :]

            low = [beyond(0, d) - own(2, d) for d in range(2)]
            high = [beyond(2, d) - own(0, d) for d in range(2)]
            for m, value in enumerate(
                (-high[0], 8.0 * high[0] - high[1], low[1] - 8.0 * low[0], low[0])
            ):
                xb[idx, pl.ds(m, levels, stride=4), :] = value

            low = [
                beyond(3, d) - q[pl.ds(first - 1 - d, levels, stride=size), :] for d in range(2)
            ]
            high = [
                beyond(1, d) - q[pl.ds(first + size + d, levels, stride=size), :] for d in range(2)
            ]
            base = idx * 2 * levels * 8
            gi[pl.ds(base, levels, stride=8), :] = low[1] - 8.0 * low[0]
            gi[pl.ds(base + 1, levels, stride=8), :] = low[0]
            base = base + levels * 8
            gi[pl.ds(base + 6, levels, stride=8), :] = -high[0]
            gi[pl.ds(base + 7, levels, stride=8), :] = 8.0 * high[0] - high[1]
        for idx in range(half):
            tt[idx] = jnp.transpose(xb[idx])
        for idx in range(half):
            start = (2 * idx + par) * block
            for k in range(levels):
                for last in range(2):
                    here = pl.ds(pl.multiple_of(start + k * size + last * (size - 8), 8), 8)
                    change = gi[pl.ds(((idx * 2 + last) * levels + k) * 8, 8), :]
                    fv[here, :] = fv[here, :] - vv[here, :] * change

        def finish(step, carry):
            idx = step // (size // 16)
            i = lax.rem(step, size // 16)
            fix = tt[idx, pl.ds(pl.multiple_of(i * 16, 16), 16), :]
            values, places = [], []
            for k in range(levels):
                row = (2 * idx + par) * block + k * size + i * 16
                here = pl.ds(pl.multiple_of(row, 16), 16)
                value = fv[here, :] - wv[here, :] * pltpu.roll(fix, size - (4 * k + 2), 1)
                if k:
                    value = value + bv[here, :] * values[-1]
                values.append(value)
                places.append(here)
            upper = values[-1]
            out[places[-1], :] = upper
            for k in range(levels - 2, -1, -1):
                upper = values[k] + rv[places[k], :] * upper
                out[places[k], :] = upper
            return carry

        lax.fori_loop(0, half * (size // 16), finish, 0, unroll=4)

    @pl.loop(0, 2)
    def _(turn):
        solve(jnp.where(bent, 1 - turn, turn))

    for key in on_edge:
        @pl.when(on_edge[key])
        def _(key=key):
            to_hub(key).wait_send()

        @pl.when(jnp.logical_not(on_edge[key]))
        def _(key=key):
            to_near(key).wait_send()

    for group, hub_device in enumerate(plan.hubs):
        @pl.when(me == hub_device)
        def _(group=group):
            for i in plan.order(group):
                to_site(group, i).wait_send()


def shards(plan, tracer, east, north, diff, seam):
    _, panels, levels, size, _ = tracer.shape
    dims = panels, levels, size
    total = panels * levels * size
    half = panels // 2
    f32, bf16 = jnp.float32, jnp.bfloat16
    anywhere = pl.BlockSpec(memory_space=pltpu.HBM)
    edge_set = pltpu.VMEM((2, 4, half, 2 * levels, size), f32)
    hub_set = pltpu.VMEM((16 * half, 2 * levels, size), f32)
    whole = pltpu.VMEM((total, size), f32)
    updated = pl.pallas_call(
        functools.partial(kernel, plan, dims),
        out_shape=pltpu.VMEM((total, size), f32),
        in_specs=[anywhere] * 6,
        out_specs=pl.BlockSpec(memory_space=pltpu.VMEM),
        scratch_shapes=[
            pltpu.SMEM((3, 4, panels), jnp.int32),
            pltpu.VMEM((2, panels * levels, 8, size), f32),
            pltpu.VMEM((total + 2 * PAD, size), f32),
            *[pltpu.VMEM((total, size), bf16)] * 3,
            *[whole] * 5,
            *[edge_set] * 3,
            *[hub_set] * 2,
            pltpu.VMEM((half * 2 * levels * 8, size), f32),
            pltpu.VMEM((half, size, size), f32),
            pltpu.VMEM((panels, size, size), f32),
            pltpu.SemaphoreType.DMA,
            pltpu.SemaphoreType.DMA((2,)),
            pltpu.SemaphoreType.DMA((panels,)),
            pltpu.SemaphoreType.DMA((panels, 3)),
            pltpu.SemaphoreType.DMA((8,)),
            pltpu.SemaphoreType.DMA((8,)),
            pltpu.SemaphoreType.DMA((16,)),
            pltpu.SemaphoreType.DMA((16,)),
        ],
        compiler_params=pltpu.CompilerParams(
            collective_id=0, has_side_effects=True, vmem_limit_bytes=40 * 1024 * 1024
        ),
        name="transport",
    )(
        *[
            pltpu.with_memory_space_constraint(value, pltpu.HBM)
            for value in (
                tracer.reshape(total, size),
                tracer.reshape(panels * levels, size, size),
                *[field.reshape(total, size) for field in (east, north, diff)],
                jnp.transpose(seam, (2, 1, 0)),
            )
        ]
    )
    return updated.reshape(tracer.shape)


def solution(mesh):
    plan = Plan(mesh.shape["tile"])
    spread = P(("groups", "tile"), None, None, None, None)
    return jax.shard_map(
        functools.partial(shards, plan),
        mesh=mesh,
        in_specs=(spread, spread, spread, spread, P()),
        out_specs=spread,
        check_vma=False,
    )
```

```python
import functools
import math

import jax
import jax.numpy as jnp
from jax import lax
from jax.experimental import pallas as pl
from jax.experimental.pallas import tpu as pltpu
from jax.sharding import PartitionSpec as P

MESH = pl.DeviceIdType.MESH
PAD = 8


class Plan:
    def __init__(self, count):
        self.count = count
        self.side = math.isqrt(count)
        self.shift = count // 2 + 1
        taken = []
        for group in range(self.side // 2):
            members = {self.site(*place) for place in self.places(group)}
            taken.append(
                next(d for d in range(5, count, 2) if d not in members and d not in taken)
            )
        self.hubs = taken

    def places(self, group):
        spots = group, self.side - 1 - group
        return [(par, edge, spot) for par in range(2) for edge in range(4) for spot in spots]

    def waves(self, group):
        homes = [self.site(*place) for place in self.places(group)]
        inner = sorted(range(len(homes)), key=lambda i: homes[i])
        first = [i for i in inner if homes[i] < self.count // 4]
        return first, [i for i in inner if i not in first]

    def site(self, par, edge, spot):
        side = self.side
        tile = (spot * side, (side - 1) * side + spot, spot * side + side - 1, spot)[edge]
        return (tile + self.shift * par) % self.count

    def hub_of(self, group):
        found = self.hubs[0]
        for i, hub in enumerate(self.hubs):
            if i:
                found = jnp.where(group == i, hub, found)
        return found


def kernel(
    plan, dims,
    tracer, slabs, east, north, diff, table, out,
    seam, rim, q, ce, cn, df, fv, wv, vv, bv, rv,
    strips, turned, ghosts, held, chosen, gi, xb, tt,
    table_sem, rim_sem, load_sem, coef_sem, send_sem, ghost_sem, held_sem, chosen_sem,
):
    panels, levels, size = dims
    count, side = plan.count, plan.side
    block = levels * size
    me = lax.axis_index("tile")
    half = panels // 2

    def device(d):
        return {"tile": d}

    tiles = [lax.rem(me + (count - plan.shift) * par, count) for par in range(2)]
    rows = [t // side for t in tiles]
    cols = [lax.rem(t, side) for t in tiles]
    on_edge, below, above_me, slot, hub, near = {}, {}, {}, {}, {}, {}
    for par in range(2):
        for edge in range(4):
            key = par, edge
            on_edge[key] = (
                cols[par] == 0, rows[par] == side - 1, cols[par] == side - 1, rows[par] == 0
            )[edge]
            spot = (rows, cols, rows, cols)[edge][par]
            group = jnp.minimum(spot, side - 1 - spot)
            slot[key] = (par * 4 + edge) * 2 + jnp.where(spot == group, 0, 1)
            hub[key] = plan.hub_of(group)
            near[key] = lax.rem(me + (count - 1, side, 1, count - side)[edge], count)
            inside = jnp.logical_not(on_edge[key])
            below[key] = jnp.logical_and(inside, near[key] < me)
            above_me[key] = jnp.logical_and(inside, near[key] > me)

    barrier = pltpu.get_barrier_semaphore()
    expected = 0
    for key in on_edge:
        expected = expected + jnp.where(jnp.logical_or(on_edge[key], below[key]), 1, 0)

        @pl.when(above_me[key])
        def _(key=key):
            pl.semaphore_signal(
                barrier, inc=1, device_id=device(near[key]), device_id_type=MESH
            )
    for group, hub_device in enumerate(plan.hubs):
        @pl.when(me == hub_device)
        def _(group=group):
            for place in plan.places(group):
                pl.semaphore_signal(
                    barrier, inc=1, device_id=device(plan.site(*place)), device_id_type=MESH
                )

    table_load = pltpu.make_async_copy(table, seam, table_sem)
    table_load.start()
    rim_loads = [
        pltpu.make_async_copy(slabs.at[:, pl.ds(start, 8), :], rim.at[i], rim_sem.at[i])
        for i, start in enumerate((0, size - 8))
    ]
    for load in rim_loads:
        load.start()
    loads = []
    for p in range(panels):
        load = pltpu.make_async_copy(
            tracer.at[pl.ds(p * block, block)], q.at[pl.ds(PAD + p * block, block)],
            load_sem.at[p],
        )
        load.start()
        loads.append(load)
    coefs = [
        pltpu.make_async_copy(
            far.at[pl.ds(p * block, block)], close.at[pl.ds(p * block, block)],
            coef_sem.at[p, i],
        )
        for p in range(panels)
        for i, (far, close) in enumerate(((east, ce), (north, cn), (diff, df)))
    ]

    zero = jnp.zeros((8, size), jnp.float32)
    q[pl.ds(0, PAD), :] = zero
    q[pl.ds(PAD + panels * block, PAD), :] = zero
    gi[...] = jnp.zeros(gi.shape, jnp.float32)
    xb[...] = jnp.zeros(xb.shape, jnp.float32)
    lane = lax.broadcasted_iota(jnp.int32, (8, size), 1)
    back = size - 1 - lax.broadcasted_iota(jnp.int32, (2 * levels, size), 1)

    def turn_strips(p, edges):
        par, idx = p % 2, p // 2
        for edge in edges:
            plain = strips[par, edge, idx]
            flipped = jnp.take_along_axis(plain, back, axis=1)
            turned[par, edge, idx] = jnp.where(seam[2, edge, p] == 1, flipped, plain)

    for load in rim_loads:
        load.wait()
    table_load.wait()
    for p in range(panels):
        par, idx = p % 2, p // 2
        for d in range(2):
            part = pl.ds(d * levels, levels)
            strips[par, 3, idx, part, :] = rim[0, pl.ds(p * levels, levels), d, :]
            strips[par, 1, idx, part, :] = rim[1, pl.ds(p * levels, levels), 7 - d, :]
    for p in range(panels):
        turn_strips(p, (1, 3))

    def to_hub(key):
        par, edge = key
        return pltpu.make_async_remote_copy(
            turned.at[par, edge], held.at[pl.ds(slot[key] * half, half)],
            send_sem.at[par * 4 + edge], held_sem.at[slot[key]],
            device_id=device(hub[key]), device_id_type=MESH,
        )

    def to_near(key):
        par, edge = key
        return pltpu.make_async_remote_copy(
            strips.at[par, edge], ghosts.at[par, (edge + 2) % 4],
            send_sem.at[par * 4 + edge], ghost_sem.at[par * 4 + (edge + 2) % 4],
            device_id=device(near[key]), device_id_type=MESH,
        )

    def arrival(par, edge):
        return pltpu.make_async_remote_copy(
            strips.at[par, edge], ghosts.at[par, edge],
            send_sem.at[par * 4 + edge], ghost_sem.at[par * 4 + edge],
            device_id=device(0), device_id_type=MESH,
        )

    def send(edges):
        keys = [(par, edge) for edge in edges for par in range(2)]
        for key in keys:
            @pl.when(on_edge[key])
            def _(key=key):
                to_hub(key).start()

        for key in keys:
            @pl.when(below[key])
            def _(key=key):
                to_near(key).start()

    pl.semaphore_wait(barrier, expected)
    send((1, 3))

    for load in loads:
        load.wait()
    for load in coefs:
        load.start()
    part_of = lane // 4
    for p in range(panels):
        for i in range(size // 8):
            packed = jnp.zeros((8, size), jnp.float32)
            for k in range(levels):
                moved = pltpu.roll(
                    q[pl.ds(PAD + p * block + k * size + i * 8, 8), :], 4 * k + 2, 1
                )
                packed = jnp.where(part_of == k, moved, packed)
            tt[p, pl.ds(i * 8, 8), :] = packed
    for p in range(panels):
        tt[p] = jnp.transpose(tt[p])
    for p in range(panels):
        par, idx = p % 2, p // 2
        for d in range(2):
            part = pl.ds(d * levels, levels)
            strips[par, 0, idx, part, :] = tt[p, pl.ds(2 + d, levels, stride=4), :]
            strips[par, 2, idx, part, :] = tt[p, pl.ds(1 - d, levels, stride=4), :]
    for p in range(panels):
        turn_strips(p, (0, 2))

    send((0, 2))

    twelfth = 1.0 / 12.0
    wide = lax.broadcasted_iota(jnp.int32, (16, size), 1)
    edge_lane = jnp.logical_or(wide < 2, wide >= size - 2)

    for p in range(panels):
        for load in coefs[3 * p : 3 * p + 3]:
            load.wait()

        def prepare(i, carry):
            before = ratio = None
            for k in range(levels):
                row = pl.multiple_of(p * block + k * size + i * 16, 16)
                here = pl.ds(row, 16)
                mid = q[pl.ds(row + PAD, 16), :]
                di = 8.0 * (q[pl.ds(row + PAD + 1, 16), :] - q[pl.ds(row + PAD - 1, 16), :]) - (
                    q[pl.ds(row + PAD + 2, 16), :] - q[pl.ds(row + PAD - 2, 16), :]
                )
                dj = 8.0 * (pltpu.roll(mid, size - 1, 1) - pltpu.roll(mid, 1, 1)) - (
                    pltpu.roll(mid, size - 2, 1) - pltpu.roll(mid, 2, 1)
                )
                e = ce[here, :].astype(jnp.float32) * twelfth
                n = cn[here, :].astype(jnp.float32) * twelfth
                c = df[here, :].astype(jnp.float32)
                pivot = 1.0 + c
                if k:
                    pivot = pivot + before * (1.0 - ratio)
                inv = 1.0 / pivot
                fv[here, :] = (mid - (e * di + n * dj)) * inv
                wv[here, :] = jnp.where(edge_lane, n * inv, 0.0)
                vv[here, :] = e * inv
                if k:
                    bv[here, :] = before * inv
                ratio = c * inv
                rv[here, :] = ratio
                before = c
            return carry

        lax.fori_loop(0, size // 16, prepare, 0)

    def send_up(around):
        for key in on_edge:
            far = near[key] - me > count // 2
            @pl.when(jnp.logical_and(above_me[key], far if around else jnp.logical_not(far)))
            def _(key=key):
                arrival(*key).wait_recv()
                to_near(key).start()

    send_up(False)

    def to_site(group, i):
        par, edge, _ = place = plan.places(group)[i]
        return pltpu.make_async_remote_copy(
            chosen.at[pl.ds(i * half, half)], ghosts.at[par, edge],
            chosen_sem.at[i], ghost_sem.at[par * 4 + edge],
            device_id=device(plan.site(*place)), device_id_type=MESH,
        )

    for group, hub_device in enumerate(plan.hubs):
        @pl.when(me == hub_device)
        def _(group=group):
            places = plan.places(group)
            for i in range(len(places)):
                pltpu.make_async_remote_copy(
                    held.at[pl.ds(i * half, half)], held.at[pl.ds(i * half, half)],
                    chosen_sem.at[i], held_sem.at[i],
                    device_id=device(0), device_id_type=MESH,
                ).wait_recv()
            first, rest = plan.waves(group)
            for i in first + [None] + rest:
                if i is None:
                    for j in first:
                        to_site(group, j).wait_send()
                    continue
                par, edge, spot = places[i]
                mirrored = int(spot != group)
                for idx in range(half):
                    far_panel, far_edge, turn = (seam[j, edge, 2 * idx + par] for j in range(3))
                    far_mirrored = mirrored + turn - 2 * mirrored * turn
                    source = ((far_panel % 2) * 4 + far_edge) * 2 + far_mirrored
                    chosen[i * half + idx] = held[source * half + far_panel // 2]
                to_site(group, i).start()

    send_up(True)

    bent = functools.reduce(jnp.logical_or, [on_edge[0, edge] for edge in range(4)])

    def solve(par):
        for edge in range(4):
            late = jnp.logical_not(jnp.where(par == 0, above_me[0, edge], above_me[1, edge]))

            @pl.when(late)
            def _(edge=edge):
                arrival(par, edge).wait_recv()

        for idx in range(half):
            p = 2 * idx + par
            first = pl.multiple_of(PAD + p * block, 8)

            def beyond(edge, d):
                return ghosts[par, edge, idx, pl.ds(d * levels, levels), :]

            def own(edge, d):
                return strips[par, edge, idx, pl.ds(d * levels, levels), :]

            low = [beyond(0, d) - own(2, d) for d in range(2)]
            high = [beyond(2, d) - own(0, d) for d in range(2)]
            for m, value in enumerate(
                (-high[0], 8.0 * high[0] - high[1], low[1] - 8.0 * low[0], low[0])
            ):
                xb[idx, pl.ds(m, levels, stride=4), :] = value

            low = [
                beyond(3, d) - q[pl.ds(first - 1 - d, levels, stride=size), :] for d in range(2)
            ]
            high = [
                beyond(1, d) - q[pl.ds(first + size + d, levels, stride=size), :] for d in range(2)
            ]
            base = idx * 2 * levels * 8
            gi[pl.ds(base, levels, stride=8), :] = low[1] - 8.0 * low[0]
            gi[pl.ds(base + 1, levels, stride=8), :] = low[0]
            base = base + levels * 8
            gi[pl.ds(base + 6, levels, stride=8), :] = -high[0]
            gi[pl.ds(base + 7, levels, stride=8), :] = 8.0 * high[0] - high[1]
        for idx in range(half):
            tt[idx] = jnp.transpose(xb[idx])
        for idx in range(half):
            start = (2 * idx + par) * block
            for k in range(levels):
                for last in range(2):
                    here = pl.ds(pl.multiple_of(start + k * size + last * (size - 8), 8), 8)
                    change = gi[pl.ds(((idx * 2 + last) * levels + k) * 8, 8), :]
                    fv[here, :] = fv[here, :] - vv[here, :] * change

        def finish(step, carry):
            idx = step // (size // 16)
            i = lax.rem(step, size // 16)
            fix = tt[idx, pl.ds(pl.multiple_of(i * 16, 16), 16), :]
            values, places = [], []
            for k in range(levels):
                row = (2 * idx + par) * block + k * size + i * 16
                here = pl.ds(pl.multiple_of(row, 16), 16)
                value = fv[here, :] - wv[here, :] * pltpu.roll(fix, size - (4 * k + 2), 1)
                if k:
                    value = value + bv[here, :] * values[-1]
                values.append(value)
                places.append(here)
            upper = values[-1]
            out[places[-1], :] = upper
            for k in range(levels - 2, -1, -1):
                upper = values[k] + rv[places[k], :] * upper
                out[places[k], :] = upper
            return carry

        lax.fori_loop(0, half * (size // 16), finish, 0, unroll=8)

    @pl.loop(0, 2)
    def _(turn):
        solve(jnp.where(bent, 1 - turn, turn))

    for key in on_edge:
        @pl.when(on_edge[key])
        def _(key=key):
            to_hub(key).wait_send()

        @pl.when(jnp.logical_not(on_edge[key]))
        def _(key=key):
            to_near(key).wait_send()

    for group, hub_device in enumerate(plan.hubs):
        @pl.when(me == hub_device)
        def _(group=group):
            for i in plan.waves(group)[1]:
                to_site(group, i).wait_send()


def shards(plan, tracer, east, north, diff, seam):
    _, panels, levels, size, _ = tracer.shape
    dims = panels, levels, size
    total = panels * levels * size
    half = panels // 2
    f32, bf16 = jnp.float32, jnp.bfloat16
    anywhere = pl.BlockSpec(memory_space=pltpu.HBM)
    edge_set = pltpu.VMEM((2, 4, half, 2 * levels, size), f32)
    hub_set = pltpu.VMEM((16 * half, 2 * levels, size), f32)
    whole = pltpu.VMEM((total, size), f32)
    updated = pl.pallas_call(
        functools.partial(kernel, plan, dims),
        out_shape=pltpu.VMEM((total, size), f32),
        in_specs=[anywhere] * 6,
        out_specs=pl.BlockSpec(memory_space=pltpu.VMEM),
        scratch_shapes=[
            pltpu.SMEM((3, 4, panels), jnp.int32),
            pltpu.VMEM((2, panels * levels, 8, size), f32),
            pltpu.VMEM((total + 2 * PAD, size), f32),
            *[pltpu.VMEM((total, size), bf16)] * 3,
            *[whole] * 5,
            *[edge_set] * 3,
            *[hub_set] * 2,
            pltpu.VMEM((half * 2 * levels * 8, size), f32),
            pltpu.VMEM((half, size, size), f32),
            pltpu.VMEM((panels, size, size), f32),
            pltpu.SemaphoreType.DMA,
            pltpu.SemaphoreType.DMA((2,)),
            pltpu.SemaphoreType.DMA((panels,)),
            pltpu.SemaphoreType.DMA((panels, 3)),
            pltpu.SemaphoreType.DMA((8,)),
            pltpu.SemaphoreType.DMA((8,)),
            pltpu.SemaphoreType.DMA((16,)),
            pltpu.SemaphoreType.DMA((16,)),
        ],
        compiler_params=pltpu.CompilerParams(
            collective_id=0, has_side_effects=True, vmem_limit_bytes=40 * 1024 * 1024
        ),
        name="transport",
    )(
        *[
            pltpu.with_memory_space_constraint(value, pltpu.HBM)
            for value in (
                tracer.reshape(total, size),
                tracer.reshape(panels * levels, size, size),
                *[field.reshape(total, size) for field in (east, north, diff)],
                jnp.transpose(seam, (2, 1, 0)),
            )
        ]
    )
    return updated.reshape(tracer.shape)


def solution(mesh):
    plan = Plan(mesh.shape["tile"])
    spread = P(("groups", "tile"), None, None, None, None)
    return jax.shard_map(
        functools.partial(shards, plan),
        mesh=mesh,
        in_specs=(spread, spread, spread, spread, P()),
        out_specs=spread,
        check_vma=False,
    )
```

```python
import functools
import math

import jax
import jax.numpy as jnp
from jax import lax
from jax.experimental import pallas as pl
from jax.experimental.pallas import tpu as pltpu
from jax.sharding import PartitionSpec as P

MESH = pl.DeviceIdType.MESH
PAD = 8


class Plan:
    def __init__(self, count):
        self.count = count
        self.side = math.isqrt(count)
        self.shift = count // 2 + 1
        taken = []
        for group in range(self.side // 2):
            members = {self.site(*place) for place in self.places(group)}
            taken.append(
                next(d for d in range(5, count, 2) if d not in members and d not in taken)
            )
        self.hubs = taken

    def places(self, group):
        spots = group, self.side - 1 - group
        return [(par, edge, spot) for par in range(2) for edge in range(4) for spot in spots]

    def waves(self, group):
        homes = [self.site(*place) for place in self.places(group)]
        inner = sorted(range(len(homes)), key=lambda i: homes[i])
        near = [i for i in inner if homes[i] < self.count // 4]
        ahead = [i for i in inner if self.count // 4 <= homes[i] < self.count // 2 + 6]
        behind = [i for i in inner if i not in near + ahead]
        return [near, ahead + behind] if group == 0 else [near, ahead, behind]

    def site(self, par, edge, spot):
        side = self.side
        tile = (spot * side, (side - 1) * side + spot, spot * side + side - 1, spot)[edge]
        return (tile + self.shift * par) % self.count

    def hub_of(self, group):
        found = self.hubs[0]
        for i, hub in enumerate(self.hubs):
            if i:
                found = jnp.where(group == i, hub, found)
        return found


def kernel(
    plan, dims,
    tracer, slabs, east, north, diff, table, out,
    seam, rim, q, ce, cn, df, fv, wv, vv, bv, rv,
    strips, turned, ghosts, held, chosen, gi, xb, tt,
    table_sem, rim_sem, load_sem, coef_sem, send_sem, ghost_sem, held_sem, chosen_sem,
):
    panels, levels, size = dims
    count, side = plan.count, plan.side
    block = levels * size
    me = lax.axis_index("tile")
    half = panels // 2

    def device(d):
        return {"tile": d}

    tiles = [lax.rem(me + (count - plan.shift) * par, count) for par in range(2)]
    rows = [t // side for t in tiles]
    cols = [lax.rem(t, side) for t in tiles]
    on_edge, below, above_me, slot, hub, near = {}, {}, {}, {}, {}, {}
    for par in range(2):
        for edge in range(4):
            key = par, edge
            on_edge[key] = (
                cols[par] == 0, rows[par] == side - 1, cols[par] == side - 1, rows[par] == 0
            )[edge]
            spot = (rows, cols, rows, cols)[edge][par]
            group = jnp.minimum(spot, side - 1 - spot)
            slot[key] = (par * 4 + edge) * 2 + jnp.where(spot == group, 0, 1)
            hub[key] = plan.hub_of(group)
            near[key] = lax.rem(me + (count - 1, side, 1, count - side)[edge], count)
            inside = jnp.logical_not(on_edge[key])
            below[key] = jnp.logical_and(inside, near[key] < me)
            above_me[key] = jnp.logical_and(inside, near[key] > me)

    barrier = pltpu.get_barrier_semaphore()
    expected = 0
    for key in on_edge:
        expected = expected + jnp.where(jnp.logical_or(on_edge[key], below[key]), 1, 0)

        @pl.when(above_me[key])
        def _(key=key):
            pl.semaphore_signal(
                barrier, inc=1, device_id=device(near[key]), device_id_type=MESH
            )
    for group, hub_device in enumerate(plan.hubs):
        @pl.when(me == hub_device)
        def _(group=group):
            for place in plan.places(group):
                pl.semaphore_signal(
                    barrier, inc=1, device_id=device(plan.site(*place)), device_id_type=MESH
                )

    table_load = pltpu.make_async_copy(table, seam, table_sem)
    table_load.start()
    rim_loads = [
        pltpu.make_async_copy(slabs.at[:, pl.ds(start, 8), :], rim.at[i], rim_sem.at[i])
        for i, start in enumerate((0, size - 8))
    ]
    for load in rim_loads:
        load.start()
    loads = []
    for p in range(panels):
        load = pltpu.make_async_copy(
            tracer.at[pl.ds(p * block, block)], q.at[pl.ds(PAD + p * block, block)],
            load_sem.at[p],
        )
        load.start()
        loads.append(load)
    coefs = [
        pltpu.make_async_copy(
            far.at[pl.ds(p * block, block)], close.at[pl.ds(p * block, block)],
            coef_sem.at[p, i],
        )
        for p in range(panels)
        for i, (far, close) in enumerate(((east, ce), (north, cn), (diff, df)))
    ]

    zero = jnp.zeros((8, size), jnp.float32)
    q[pl.ds(0, PAD), :] = zero
    q[pl.ds(PAD + panels * block, PAD), :] = zero
    gi[...] = jnp.zeros(gi.shape, jnp.float32)
    xb[...] = jnp.zeros(xb.shape, jnp.float32)
    lane = lax.broadcasted_iota(jnp.int32, (8, size), 1)
    back = size - 1 - lax.broadcasted_iota(jnp.int32, (2 * levels, size), 1)

    def turn_strips(p, edges):
        par, idx = p % 2, p // 2
        for edge in edges:
            plain = strips[par, edge, idx]
            flipped = jnp.take_along_axis(plain, back, axis=1)
            turned[par, edge, idx] = jnp.where(seam[2, edge, p] == 1, flipped, plain)

    for load in rim_loads:
        load.wait()
    table_load.wait()
    for p in range(panels):
        par, idx = p % 2, p // 2
        for d in range(2):
            part = pl.ds(d * levels, levels)
            strips[par, 3, idx, part, :] = rim[0, pl.ds(p * levels, levels), d, :]
            strips[par, 1, idx, part, :] = rim[1, pl.ds(p * levels, levels), 7 - d, :]
    for p in range(panels):
        turn_strips(p, (1, 3))

    def to_hub(key):
        par, edge = key
        return pltpu.make_async_remote_copy(
            turned.at[par, edge], held.at[pl.ds(slot[key] * half, half)],
            send_sem.at[par * 4 + edge], held_sem.at[slot[key]],
            device_id=device(hub[key]), device_id_type=MESH,
        )

    def to_near(key):
        par, edge = key
        return pltpu.make_async_remote_copy(
            strips.at[par, edge], ghosts.at[par, (edge + 2) % 4],
            send_sem.at[par * 4 + edge], ghost_sem.at[par * 4 + (edge + 2) % 4],
            device_id=device(near[key]), device_id_type=MESH,
        )

    def arrival(par, edge):
        return pltpu.make_async_remote_copy(
            strips.at[par, edge], ghosts.at[par, edge],
            send_sem.at[par * 4 + edge], ghost_sem.at[par * 4 + edge],
            device_id=device(0), device_id_type=MESH,
        )

    def send(edges):
        keys = [(par, edge) for edge in edges for par in range(2)]
        for key in keys:
            @pl.when(on_edge[key])
            def _(key=key):
                to_hub(key).start()

        for key in keys:
            @pl.when(below[key])
            def _(key=key):
                to_near(key).start()

    pl.semaphore_wait(barrier, expected)
    send((1, 3))

    for load in loads:
        load.wait()
    for load in coefs:
        load.start()
    part_of = lane // 4
    for p in range(panels):
        for i in range(size // 8):
            packed = jnp.zeros((8, size), jnp.float32)
            for k in range(levels):
                moved = pltpu.roll(
                    q[pl.ds(PAD + p * block + k * size + i * 8, 8), :], 4 * k + 2, 1
                )
                packed = jnp.where(part_of == k, moved, packed)
            tt[p, pl.ds(i * 8, 8), :] = packed
    for p in range(panels):
        tt[p] = jnp.transpose(tt[p])
    for p in range(panels):
        par, idx = p % 2, p // 2
        for d in range(2):
            part = pl.ds(d * levels, levels)
            strips[par, 0, idx, part, :] = tt[p, pl.ds(2 + d, levels, stride=4), :]
            strips[par, 2, idx, part, :] = tt[p, pl.ds(1 - d, levels, stride=4), :]
    for p in range(panels):
        turn_strips(p, (0, 2))

    send((0, 2))

    twelfth = 1.0 / 12.0
    wide = lax.broadcasted_iota(jnp.int32, (16, size), 1)
    edge_lane = jnp.logical_or(wide < 2, wide >= size - 2)

    for p in range(panels):
        for load in coefs[3 * p : 3 * p + 3]:
            load.wait()

        def prepare(i, carry):
            before = ratio = None
            for k in range(levels):
                row = pl.multiple_of(p * block + k * size + i * 16, 16)
                here = pl.ds(row, 16)
                mid = q[pl.ds(row + PAD, 16), :]
                di = 8.0 * (q[pl.ds(row + PAD + 1, 16), :] - q[pl.ds(row + PAD - 1, 16), :]) - (
                    q[pl.ds(row + PAD + 2, 16), :] - q[pl.ds(row + PAD - 2, 16), :]
                )
                dj = 8.0 * (pltpu.roll(mid, size - 1, 1) - pltpu.roll(mid, 1, 1)) - (
                    pltpu.roll(mid, size - 2, 1) - pltpu.roll(mid, 2, 1)
                )
                e = ce[here, :].astype(jnp.float32) * twelfth
                n = cn[here, :].astype(jnp.float32) * twelfth
                c = df[here, :].astype(jnp.float32)
                pivot = 1.0 + c
                if k:
                    pivot = pivot + before * (1.0 - ratio)
                inv = 1.0 / pivot
                fv[here, :] = (mid - (e * di + n * dj)) * inv
                wv[here, :] = jnp.where(edge_lane, n * inv, 0.0)
                vv[here, :] = e * inv
                if k:
                    bv[here, :] = before * inv
                ratio = c * inv
                rv[here, :] = ratio
                before = c
            return carry

        lax.fori_loop(0, size // 16, prepare, 0)

    def send_up(around):
        for key in on_edge:
            far = near[key] - me > count // 2
            @pl.when(jnp.logical_and(above_me[key], far if around else jnp.logical_not(far)))
            def _(key=key):
                arrival(*key).wait_recv()
                to_near(key).start()

    send_up(False)

    def to_site(group, i):
        par, edge, _ = place = plan.places(group)[i]
        return pltpu.make_async_remote_copy(
            chosen.at[pl.ds(i * half, half)], ghosts.at[par, edge],
            chosen_sem.at[i], ghost_sem.at[par * 4 + edge],
            device_id=device(plan.site(*place)), device_id_type=MESH,
        )

    for group, hub_device in enumerate(plan.hubs):
        @pl.when(me == hub_device)
        def _(group=group):
            places = plan.places(group)
            for i in range(len(places)):
                pltpu.make_async_remote_copy(
                    held.at[pl.ds(i * half, half)], held.at[pl.ds(i * half, half)],
                    chosen_sem.at[i], held_sem.at[i],
                    device_id=device(0), device_id_type=MESH,
                ).wait_recv()
            waves = plan.waves(group)
            steps = [(number, i) for number, wave in enumerate(waves) for i in wave]
            sent = 0
            for number, i in steps:
                while sent < number:
                    for j in waves[sent]:
                        to_site(group, j).wait_send()
                    sent += 1
                par, edge, spot = places[i]
                mirrored = int(spot != group)
                for idx in range(half):
                    far_panel, far_edge, turn = (seam[j, edge, 2 * idx + par] for j in range(3))
                    far_mirrored = mirrored + turn - 2 * mirrored * turn
                    source = ((far_panel % 2) * 4 + far_edge) * 2 + far_mirrored
                    chosen[i * half + idx] = held[source * half + far_panel // 2]
                to_site(group, i).start()

    send_up(True)

    bent = functools.reduce(jnp.logical_or, [on_edge[0, edge] for edge in range(4)])

    def solve(par):
        for edge in range(4):
            late = jnp.logical_not(jnp.where(par == 0, above_me[0, edge], above_me[1, edge]))

            @pl.when(late)
            def _(edge=edge):
                arrival(par, edge).wait_recv()

        for idx in range(half):
            p = 2 * idx + par
            first = pl.multiple_of(PAD + p * block, 8)

            def beyond(edge, d):
                return ghosts[par, edge, idx, pl.ds(d * levels, levels), :]

            def own(edge, d):
                return strips[par, edge, idx, pl.ds(d * levels, levels), :]

            low = [beyond(0, d) - own(2, d) for d in range(2)]
            high = [beyond(2, d) - own(0, d) for d in range(2)]
            for m, value in enumerate(
                (-high[0], 8.0 * high[0] - high[1], low[1] - 8.0 * low[0], low[0])
            ):
                xb[idx, pl.ds(m, levels, stride=4), :] = value

            low = [
                beyond(3, d) - q[pl.ds(first - 1 - d, levels, stride=size), :] for d in range(2)
            ]
            high = [
                beyond(1, d) - q[pl.ds(first + size + d, levels, stride=size), :] for d in range(2)
            ]
            base = idx * 2 * levels * 8
            gi[pl.ds(base, levels, stride=8), :] = low[1] - 8.0 * low[0]
            gi[pl.ds(base + 1, levels, stride=8), :] = low[0]
            base = base + levels * 8
            gi[pl.ds(base + 6, levels, stride=8), :] = -high[0]
            gi[pl.ds(base + 7, levels, stride=8), :] = 8.0 * high[0] - high[1]
        for idx in range(half):
            tt[idx] = jnp.transpose(xb[idx])
        for idx in range(half):
            start = (2 * idx + par) * block
            for k in range(levels):
                for last in range(2):
                    here = pl.ds(pl.multiple_of(start + k * size + last * (size - 8), 8), 8)
                    change = gi[pl.ds(((idx * 2 + last) * levels + k) * 8, 8), :]
                    fv[here, :] = fv[here, :] - vv[here, :] * change

        def finish(step, carry):
            idx = step // (size // 16)
            i = lax.rem(step, size // 16)
            fix = tt[idx, pl.ds(pl.multiple_of(i * 16, 16), 16), :]
            values, places = [], []
            for k in range(levels):
                row = (2 * idx + par) * block + k * size + i * 16
                here = pl.ds(pl.multiple_of(row, 16), 16)
                value = fv[here, :] - wv[here, :] * pltpu.roll(fix, size - (4 * k + 2), 1)
                if k:
                    value = value + bv[here, :] * values[-1]
                values.append(value)
                places.append(here)
            upper = values[-1]
            out[places[-1], :] = upper
            for k in range(levels - 2, -1, -1):
                upper = values[k] + rv[places[k], :] * upper
                out[places[k], :] = upper
            return carry

        lax.fori_loop(0, half * (size // 16), finish, 0, unroll=8)

    @pl.loop(0, 2)
    def _(turn):
        solve(jnp.where(bent, 1 - turn, turn))

    for key in on_edge:
        @pl.when(on_edge[key])
        def _(key=key):
            to_hub(key).wait_send()

        @pl.when(jnp.logical_not(on_edge[key]))
        def _(key=key):
            to_near(key).wait_send()

    for group, hub_device in enumerate(plan.hubs):
        @pl.when(me == hub_device)
        def _(group=group):
            for i in plan.waves(group)[-1]:
                to_site(group, i).wait_send()


def shards(plan, tracer, east, north, diff, seam):
    _, panels, levels, size, _ = tracer.shape
    dims = panels, levels, size
    total = panels * levels * size
    half = panels // 2
    f32, bf16 = jnp.float32, jnp.bfloat16
    anywhere = pl.BlockSpec(memory_space=pltpu.HBM)
    edge_set = pltpu.VMEM((2, 4, half, 2 * levels, size), f32)
    hub_set = pltpu.VMEM((16 * half, 2 * levels, size), f32)
    whole = pltpu.VMEM((total, size), f32)
    updated = pl.pallas_call(
        functools.partial(kernel, plan, dims),
        out_shape=pltpu.VMEM((total, size), f32),
        in_specs=[anywhere] * 6,
        out_specs=pl.BlockSpec(memory_space=pltpu.VMEM),
        scratch_shapes=[
            pltpu.SMEM((3, 4, panels), jnp.int32),
            pltpu.VMEM((2, panels * levels, 8, size), f32),
            pltpu.VMEM((total + 2 * PAD, size), f32),
            *[pltpu.VMEM((total, size), bf16)] * 3,
            *[whole] * 5,
            *[edge_set] * 3,
            *[hub_set] * 2,
            pltpu.VMEM((half * 2 * levels * 8, size), f32),
            pltpu.VMEM((half, size, size), f32),
            pltpu.VMEM((panels, size, size), f32),
            pltpu.SemaphoreType.DMA,
            pltpu.SemaphoreType.DMA((2,)),
            pltpu.SemaphoreType.DMA((panels,)),
            pltpu.SemaphoreType.DMA((panels, 3)),
            pltpu.SemaphoreType.DMA((8,)),
            pltpu.SemaphoreType.DMA((8,)),
            pltpu.SemaphoreType.DMA((16,)),
            pltpu.SemaphoreType.DMA((16,)),
        ],
        compiler_params=pltpu.CompilerParams(
            collective_id=0, has_side_effects=True, vmem_limit_bytes=40 * 1024 * 1024
        ),
        name="transport",
    )(
        *[
            pltpu.with_memory_space_constraint(value, pltpu.HBM)
            for value in (
                tracer.reshape(total, size),
                tracer.reshape(panels * levels, size, size),
                *[field.reshape(total, size) for field in (east, north, diff)],
                jnp.transpose(seam, (2, 1, 0)),
            )
        ]
    )
    return updated.reshape(tracer.shape)


def solution(mesh):
    plan = Plan(mesh.shape["tile"])
    spread = P(("groups", "tile"), None, None, None, None)
    return jax.shard_map(
        functools.partial(shards, plan),
        mesh=mesh,
        in_specs=(spread, spread, spread, spread, P()),
        out_specs=spread,
        check_vma=False,
    )
```

```python
import functools
import math

import jax
import jax.numpy as jnp
from jax import lax
from jax.experimental import pallas as pl
from jax.experimental.pallas import tpu as pltpu
from jax.sharding import PartitionSpec as P

MESH = pl.DeviceIdType.MESH
PAD = 8


class Plan:
    def __init__(self, count):
        self.count = count
        self.side = math.isqrt(count)
        self.shift = count // 2 + 1
        taken = []
        for group in range(self.side // 2):
            members = {self.site(*place) for place in self.places(group)}
            taken.append(
                next(d for d in range(5, count, 2) if d not in members and d not in taken)
            )
        self.hubs = taken

    def places(self, group):
        spots = group, self.side - 1 - group
        return [(par, edge, spot) for par in range(2) for edge in range(4) for spot in spots]

    def waves(self, group):
        homes = [self.site(*place) for place in self.places(group)]
        inner = sorted(range(len(homes)), key=lambda i: homes[i])
        near = [i for i in inner if homes[i] < self.count // 4]
        ahead = [i for i in inner if self.count // 4 <= homes[i] < self.count // 2 + 6]
        behind = [i for i in inner if i not in near + ahead]
        return [near, ahead + behind] if group == 0 else [near, ahead, behind]

    def site(self, par, edge, spot):
        side = self.side
        tile = (spot * side, (side - 1) * side + spot, spot * side + side - 1, spot)[edge]
        return (tile + self.shift * par) % self.count

    def hub_of(self, group):
        found = self.hubs[0]
        for i, hub in enumerate(self.hubs):
            if i:
                found = jnp.where(group == i, hub, found)
        return found


def kernel(
    plan, dims,
    tracer, slabs, east, north, diff, table, out,
    seam, rim, q, ce, cn, df, fv, wv, vv, bv, rv,
    strips, turned, ghosts, held, chosen, gi, xb, tt,
    table_sem, rim_sem, load_sem, coef_sem, send_sem, ghost_sem, held_sem, chosen_sem,
):
    panels, levels, size = dims
    count, side = plan.count, plan.side
    block = levels * size
    me = lax.axis_index("tile")
    half = panels // 2

    def device(d):
        return {"tile": d}

    tiles = [lax.rem(me + (count - plan.shift) * par, count) for par in range(2)]
    rows = [t // side for t in tiles]
    cols = [lax.rem(t, side) for t in tiles]
    on_edge, below, above_me, slot, hub, near = {}, {}, {}, {}, {}, {}
    for par in range(2):
        for edge in range(4):
            key = par, edge
            on_edge[key] = (
                cols[par] == 0, rows[par] == side - 1, cols[par] == side - 1, rows[par] == 0
            )[edge]
            spot = (rows, cols, rows, cols)[edge][par]
            group = jnp.minimum(spot, side - 1 - spot)
            slot[key] = (par * 4 + edge) * 2 + jnp.where(spot == group, 0, 1)
            hub[key] = plan.hub_of(group)
            near[key] = lax.rem(me + (count - 1, side, 1, count - side)[edge], count)
            inside = jnp.logical_not(on_edge[key])
            below[key] = jnp.logical_and(inside, near[key] < me)
            above_me[key] = jnp.logical_and(inside, near[key] > me)

    barrier = pltpu.get_barrier_semaphore()
    expected = 0
    for key in on_edge:
        expected = expected + jnp.where(jnp.logical_or(on_edge[key], below[key]), 1, 0)

        @pl.when(above_me[key])
        def _(key=key):
            pl.semaphore_signal(
                barrier, inc=1, device_id=device(near[key]), device_id_type=MESH
            )
    for group, hub_device in enumerate(plan.hubs):
        @pl.when(me == hub_device)
        def _(group=group):
            for place in plan.places(group):
                pl.semaphore_signal(
                    barrier, inc=1, device_id=device(plan.site(*place)), device_id_type=MESH
                )

    table_load = pltpu.make_async_copy(table, seam, table_sem)
    table_load.start()
    rim_loads = [
        pltpu.make_async_copy(slabs.at[:, pl.ds(start, 8), :], rim.at[i], rim_sem.at[i])
        for i, start in enumerate((0, size - 8))
    ]
    for load in rim_loads:
        load.start()
    loads = []
    for p in range(panels):
        load = pltpu.make_async_copy(
            tracer.at[pl.ds(p * block, block)], q.at[pl.ds(PAD + p * block, block)],
            load_sem.at[p],
        )
        load.start()
        loads.append(load)
    coefs = [
        pltpu.make_async_copy(
            far.at[pl.ds(p * block, block)], close.at[pl.ds(p * block, block)],
            coef_sem.at[p, i],
        )
        for p in range(panels)
        for i, (far, close) in enumerate(((east, ce), (north, cn), (diff, df)))
    ]

    zero = jnp.zeros((8, size), jnp.float32)
    q[pl.ds(0, PAD), :] = zero
    q[pl.ds(PAD + panels * block, PAD), :] = zero
    gi[...] = jnp.zeros(gi.shape, jnp.float32)
    xb[...] = jnp.zeros(xb.shape, jnp.float32)
    lane = lax.broadcasted_iota(jnp.int32, (8, size), 1)
    back = size - 1 - lax.broadcasted_iota(jnp.int32, (2 * levels, size), 1)

    def turn_strips(p, edges):
        par, idx = p % 2, p // 2
        for edge in edges:
            plain = strips[par, edge, idx]
            flipped = jnp.take_along_axis(plain, back, axis=1)
            turned[par, edge, idx] = jnp.where(seam[2, edge, p] == 1, flipped, plain)

    for load in rim_loads:
        load.wait()
    table_load.wait()
    for p in range(panels):
        par, idx = p % 2, p // 2
        for d in range(2):
            part = pl.ds(d * levels, levels)
            strips[par, 3, idx, part, :] = rim[0, pl.ds(p * levels, levels), d, :]
            strips[par, 1, idx, part, :] = rim[1, pl.ds(p * levels, levels), 7 - d, :]
    for p in range(panels):
        turn_strips(p, (1, 3))

    def to_hub(key):
        par, edge = key
        return pltpu.make_async_remote_copy(
            turned.at[par, edge], held.at[pl.ds(slot[key] * half, half)],
            send_sem.at[par * 4 + edge], held_sem.at[slot[key]],
            device_id=device(hub[key]), device_id_type=MESH,
        )

    def to_near(key):
        par, edge = key
        return pltpu.make_async_remote_copy(
            strips.at[par, edge], ghosts.at[par, (edge + 2) % 4],
            send_sem.at[par * 4 + edge], ghost_sem.at[par * 4 + (edge + 2) % 4],
            device_id=device(near[key]), device_id_type=MESH,
        )

    def arrival(par, edge):
        return pltpu.make_async_remote_copy(
            strips.at[par, edge], ghosts.at[par, edge],
            send_sem.at[par * 4 + edge], ghost_sem.at[par * 4 + edge],
            device_id=device(0), device_id_type=MESH,
        )

    def send(edges):
        keys = [(par, edge) for edge in edges for par in range(2)]
        for key in keys:
            @pl.when(on_edge[key])
            def _(key=key):
                to_hub(key).start()

        for key in keys:
            @pl.when(below[key])
            def _(key=key):
                to_near(key).start()

    pl.semaphore_wait(barrier, expected)
    send((1, 3))

    for load in loads:
        load.wait()
    for load in coefs:
        load.start()
    part_of = lane // 4
    for p in range(panels):
        for i in range(size // 8):
            packed = jnp.zeros((8, size), jnp.float32)
            for k in range(levels):
                moved = pltpu.roll(
                    q[pl.ds(PAD + p * block + k * size + i * 8, 8), :], 4 * k + 2, 1
                )
                packed = jnp.where(part_of == k, moved, packed)
            tt[p, pl.ds(i * 8, 8), :] = packed
    for p in range(panels):
        tt[p] = jnp.transpose(tt[p])
    for p in range(panels):
        par, idx = p % 2, p // 2
        for d in range(2):
            part = pl.ds(d * levels, levels)
            strips[par, 0, idx, part, :] = tt[p, pl.ds(2 + d, levels, stride=4), :]
            strips[par, 2, idx, part, :] = tt[p, pl.ds(1 - d, levels, stride=4), :]
    for p in range(panels):
        turn_strips(p, (0, 2))

    send((0, 2))

    twelfth = 1.0 / 12.0
    wide = lax.broadcasted_iota(jnp.int32, (16, size), 1)
    edge_lane = jnp.logical_or(wide < 2, wide >= size - 2)

    for p in range(panels):
        for load in coefs[3 * p : 3 * p + 3]:
            load.wait()

        def prepare(i, carry):
            before = ratio = None
            for k in range(levels):
                row = pl.multiple_of(p * block + k * size + i * 16, 16)
                here = pl.ds(row, 16)
                mid = q[pl.ds(row + PAD, 16), :]
                di = 8.0 * (q[pl.ds(row + PAD + 1, 16), :] - q[pl.ds(row + PAD - 1, 16), :]) - (
                    q[pl.ds(row + PAD + 2, 16), :] - q[pl.ds(row + PAD - 2, 16), :]
                )
                dj = 8.0 * (pltpu.roll(mid, size - 1, 1) - pltpu.roll(mid, 1, 1)) - (
                    pltpu.roll(mid, size - 2, 1) - pltpu.roll(mid, 2, 1)
                )
                e = ce[here, :].astype(jnp.float32) * twelfth
                n = cn[here, :].astype(jnp.float32) * twelfth
                c = df[here, :].astype(jnp.float32)
                pivot = 1.0 + c
                if k:
                    pivot = pivot + before * (1.0 - ratio)
                inv = 1.0 / pivot
                fv[here, :] = (mid - (e * di + n * dj)) * inv
                wv[here, :] = jnp.where(edge_lane, n * inv, 0.0)
                vv[here, :] = e * inv
                if k:
                    bv[here, :] = before * inv
                ratio = c * inv
                rv[here, :] = ratio
                before = c
            return carry

        lax.fori_loop(0, size // 16, prepare, 0)

    def send_up(around):
        for key in on_edge:
            far = near[key] - me > count // 2
            @pl.when(jnp.logical_and(above_me[key], far if around else jnp.logical_not(far)))
            def _(key=key):
                arrival(*key).wait_recv()
                to_near(key).start()

    send_up(False)

    def to_site(group, i):
        par, edge, _ = place = plan.places(group)[i]
        return pltpu.make_async_remote_copy(
            chosen.at[pl.ds(i * half, half)], ghosts.at[par, edge],
            chosen_sem.at[i], ghost_sem.at[par * 4 + edge],
            device_id=device(plan.site(*place)), device_id_type=MESH,
        )

    for group, hub_device in enumerate(plan.hubs):
        @pl.when(me == hub_device)
        def _(group=group):
            places = plan.places(group)
            for i in range(len(places)):
                pltpu.make_async_remote_copy(
                    held.at[pl.ds(i * half, half)], held.at[pl.ds(i * half, half)],
                    chosen_sem.at[i], held_sem.at[i],
                    device_id=device(0), device_id_type=MESH,
                ).wait_recv()
            waves = plan.waves(group)
            steps = [(number, i) for number, wave in enumerate(waves) for i in wave]
            sent = 0
            for number, i in steps:
                while sent < number:
                    for j in waves[sent]:
                        to_site(group, j).wait_send()
                    sent += 1
                par, edge, spot = places[i]
                mirrored = int(spot != group)
                for idx in range(half):
                    far_panel, far_edge, turn = (seam[j, edge, 2 * idx + par] for j in range(3))
                    far_mirrored = mirrored + turn - 2 * mirrored * turn
                    source = ((far_panel % 2) * 4 + far_edge) * 2 + far_mirrored
                    chosen[i * half + idx] = held[source * half + far_panel // 2]
                to_site(group, i).start()

    send_up(True)

    bent = functools.reduce(jnp.logical_or, [on_edge[0, edge] for edge in range(4)])

    def solve(par):
        for edge in range(4):
            late = jnp.logical_not(jnp.where(par == 0, above_me[0, edge], above_me[1, edge]))

            @pl.when(late)
            def _(edge=edge):
                arrival(par, edge).wait_recv()

        for idx in range(half):
            p = 2 * idx + par
            first = pl.multiple_of(PAD + p * block, 8)

            def beyond(edge, d):
                return ghosts[par, edge, idx, pl.ds(d * levels, levels), :]

            def own(edge, d):
                return strips[par, edge, idx, pl.ds(d * levels, levels), :]

            low = [beyond(0, d) - own(2, d) for d in range(2)]
            high = [beyond(2, d) - own(0, d) for d in range(2)]
            for m, value in enumerate(
                (-high[0], 8.0 * high[0] - high[1], low[1] - 8.0 * low[0], low[0])
            ):
                xb[idx, pl.ds(m, levels, stride=4), :] = value

            low = [
                beyond(3, d) - q[pl.ds(first - 1 - d, levels, stride=size), :] for d in range(2)
            ]
            high = [
                beyond(1, d) - q[pl.ds(first + size + d, levels, stride=size), :] for d in range(2)
            ]
            base = idx * 2 * levels * 8
            gi[pl.ds(base, levels, stride=8), :] = low[1] - 8.0 * low[0]
            gi[pl.ds(base + 1, levels, stride=8), :] = low[0]
            base = base + levels * 8
            gi[pl.ds(base + 6, levels, stride=8), :] = -high[0]
            gi[pl.ds(base + 7, levels, stride=8), :] = 8.0 * high[0] - high[1]
        for idx in range(half):
            tt[idx] = jnp.transpose(xb[idx])
        for idx in range(half):
            start = (2 * idx + par) * block
            for k in range(levels):
                for last in range(2):
                    here = pl.ds(pl.multiple_of(start + k * size + last * (size - 8), 8), 8)
                    change = gi[pl.ds(((idx * 2 + last) * levels + k) * 8, 8), :]
                    fv[here, :] = fv[here, :] - vv[here, :] * change

        def finish(step, carry):
            idx = step // (size // 16)
            i = lax.rem(step, size // 16)
            fix = tt[idx, pl.ds(pl.multiple_of(i * 16, 16), 16), :]
            values, places = [], []
            for k in range(levels):
                row = (2 * idx + par) * block + k * size + i * 16
                here = pl.ds(pl.multiple_of(row, 16), 16)
                value = fv[here, :] - wv[here, :] * pltpu.roll(fix, size - (4 * k + 2), 1)
                if k:
                    value = value + bv[here, :] * values[-1]
                values.append(value)
                places.append(here)
            upper = values[-1]
            out[places[-1], :] = upper
            for k in range(levels - 2, -1, -1):
                upper = values[k] + rv[places[k], :] * upper
                out[places[k], :] = upper
            return carry

        lax.fori_loop(0, half * (size // 16), finish, 0, unroll=8)

    @pl.loop(0, 2)
    def _(turn):
        solve(jnp.where(bent, 1 - turn, turn))

    for key in on_edge:
        @pl.when(on_edge[key])
        def _(key=key):
            to_hub(key).wait_send()

        @pl.when(jnp.logical_not(on_edge[key]))
        def _(key=key):
            to_near(key).wait_send()

    for group, hub_device in enumerate(plan.hubs):
        @pl.when(me == hub_device)
        def _(group=group):
            for i in plan.waves(group)[-1]:
                to_site(group, i).wait_send()


def shards(plan, tracer, east, north, diff, seam):
    _, panels, levels, size, _ = tracer.shape
    dims = panels, levels, size
    total = panels * levels * size
    half = panels // 2
    f32, bf16 = jnp.float32, jnp.bfloat16
    anywhere = pl.BlockSpec(memory_space=pltpu.HBM)
    edge_set = pltpu.VMEM((2, 4, half, 2 * levels, size), f32)
    hub_set = pltpu.VMEM((16 * half, 2 * levels, size), f32)
    whole = pltpu.VMEM((total, size), f32)
    updated = pl.pallas_call(
        functools.partial(kernel, plan, dims),
        out_shape=pltpu.VMEM((total, size), f32),
        in_specs=[anywhere] * 6,
        out_specs=pl.BlockSpec(memory_space=pltpu.VMEM),
        scratch_shapes=[
            pltpu.SMEM((3, 4, panels), jnp.int32),
            pltpu.VMEM((2, panels * levels, 8, size), f32),
            pltpu.VMEM((total + PAD + 2 * size, size), f32),
            *[pltpu.VMEM((total, size), bf16)] * 3,
            *[whole] * 5,
            *[edge_set] * 3,
            *[hub_set] * 2,
            pltpu.VMEM(((half * 2 + 1) * levels * 8, size), f32),
            pltpu.VMEM((half, size, size), f32),
            pltpu.VMEM((panels, size, size), f32),
            pltpu.SemaphoreType.DMA,
            pltpu.SemaphoreType.DMA((2,)),
            pltpu.SemaphoreType.DMA((panels,)),
            pltpu.SemaphoreType.DMA((panels, 3)),
            pltpu.SemaphoreType.DMA((8,)),
            pltpu.SemaphoreType.DMA((8,)),
            pltpu.SemaphoreType.DMA((16,)),
            pltpu.SemaphoreType.DMA((16,)),
        ],
        compiler_params=pltpu.CompilerParams(
            collective_id=0, has_side_effects=True, vmem_limit_bytes=40 * 1024 * 1024
        ),
        name="transport",
    )(
        *[
            pltpu.with_memory_space_constraint(value, pltpu.HBM)
            for value in (
                tracer.reshape(total, size),
                tracer.reshape(panels * levels, size, size),
                *[field.reshape(total, size) for field in (east, north, diff)],
                jnp.transpose(seam, (2, 1, 0)),
            )
        ]
    )
    return updated.reshape(tracer.shape)


def solution(mesh):
    plan = Plan(mesh.shape["tile"])
    spread = P(("groups", "tile"), None, None, None, None)
    return jax.shard_map(
        functools.partial(shards, plan),
        mesh=mesh,
        in_specs=(spread, spread, spread, spread, P()),
        out_specs=spread,
        check_vma=False,
    )
```
